32 devices in a mesh: walk: 8 (over z, x), chol: 4 (over y, core).
Axes of the slice: x: 2, y: 2, z: 4, core: 2. Of those that a mesh axis runs over, the one named last changes fastest.
Arguments:
- orbitals: bfloat16 [8, 400, 2048], P('walk', None, 'chol'), may hold values from -4 to 4
- intersection_inv: bfloat16 [8, 400, 400], P('walk'), may hold values from -0.18 to 0.18
- interp: bfloat16 [2048, 2048], P(None, 'chol'), may hold values from -0.079549513 to 0.079549513
- occ_interp: bfloat16 [400, 2048], P(None, 'chol'), may hold values from -0.18 to 0.18
- chol_factors: bfloat16 [2048, 2048], P('chol', 'walk'), may hold values from -2 to 2
- fields: float32 [8, 2048], P(None, 'walk'), may hold values from -4 to 4
Outputs:
- new_orbitals: bfloat16 [8, 400, 2048], P('walk', None, 'chol')
- force_bias: float32 [8, 2048], P(None, 'walk')
The draws below stay inside these ranges and needn't reach their ends.
All inputs are finite; a program needn't handle non-finite values.
Results may differ from the reference program's by a relative error of at most 0.017.
Values may be sent and summed in bfloat16 or wider, within the bound.
A program may use at most 64 MiB of HBM per device.

```python
import jax
import jax.numpy as jnp
from jax import lax

BASIS_SIZE = 2048
ELECTRONS = 400
PTS_DEV = 512
TERMS = 4
POINTS = 2048
VECTORS = 2048
WALKERS = 8
N_CHOL = 4


def bounded_values(key, shape, deviation):
    base = jax.random.truncated_normal(key, -3.5, 3.5, shape, jnp.float32)
    return base * deviation


def draw_orbitals(key, part):
    values = bounded_values(jax.random.fold_in(key, 11), (WALKERS, ELECTRONS, BASIS_SIZE), 1.0)
    return values.astype(jnp.bfloat16)


def draw_intersection_inv(key, part):
    deviation = 1.0 / jnp.sqrt(jnp.float32(ELECTRONS))
    values = bounded_values(jax.random.fold_in(key, 13), (WALKERS, ELECTRONS, ELECTRONS), deviation)
    return values.astype(jnp.bfloat16)


def draw_interp(key, part):
    deviation = 1.0 / jnp.sqrt(jnp.float32(BASIS_SIZE))
    values = bounded_values(jax.random.fold_in(key, 17), (BASIS_SIZE, POINTS), deviation)
    return values.astype(jnp.bfloat16)


def draw_occ_interp(key, part):
    deviation = 1.0 / jnp.sqrt(jnp.float32(ELECTRONS))
    values = bounded_values(jax.random.fold_in(key, 19), (ELECTRONS, POINTS), deviation)
    return values.astype(jnp.bfloat16)


def draw_fields(key, part):
    return bounded_values(jax.random.fold_in(key, 23), (WALKERS, VECTORS), 1.0)


def draw_chol_factors(key, part):
    first_key, second_key = jax.random.split(jax.random.fold_in(key, 7))
    column = jnp.arange(VECTORS).astype(jnp.float32) / VECTORS
    spread = jax.random.uniform(second_key, (VECTORS,), jnp.float32)
    column_scale = 0.2 * 10.0 ** (0.5 * column + 0.5 * spread)
    base = jax.random.truncated_normal(first_key, -4.0, 4.0, (POINTS, VECTORS), jnp.float32)
    normalizer = 0.75 * jnp.sqrt(jnp.float32(BASIS_SIZE) / (jnp.float32(POINTS) * jnp.float32(VECTORS)))
    values = base * column_scale[None, :] * normalizer
    return values.astype(jnp.bfloat16)


def setup_inputs(seed: int = 0) -> dict:
    key_of = jax.random.split(jax.random.key(seed), 7)
    return {
        "orbitals": draw_orbitals(jax.random.fold_in(key_of[6], 71), 0),
        "intersection_inv": draw_intersection_inv(jax.random.fold_in(key_of[6], 71), 0),
        "interp": draw_interp(jax.random.fold_in(key_of[6], 71), 0),
        "occ_interp": draw_occ_interp(jax.random.fold_in(key_of[6], 71), 0),
        "chol_factors": draw_chol_factors(jax.random.fold_in(key_of[6], 71), 0),
        "fields": draw_fields(jax.random.fold_in(key_of[6], 71), 0),
    }


time_root = 2.2


def propagate(orbit, inverse, field_row, interp, occ_interp, chol_factors):
    green = jnp.dot(inverse, orbit, preferred_element_type=jnp.float32).astype(jnp.bfloat16)
    projected = jnp.dot(green, interp, preferred_element_type=jnp.float32)
    weights = jnp.sum(occ_interp.astype(jnp.float32) * projected, axis=0)
    factors = chol_factors.astype(jnp.float32)
    bias = jnp.dot(weights, factors, precision=lax.Precision.HIGHEST)
    coeff = time_root * (field_row - bias)
    scales = jnp.dot(factors, coeff, precision=lax.Precision.HIGHEST)
    total = orbit.astype(jnp.float32)
    term = orbit
    for order in range(1, TERMS + 1):
        product = jnp.dot(term, interp, preferred_element_type=jnp.float32)
        mixed = (product * scales[None, :] / order).astype(jnp.bfloat16)
        summed = jnp.zeros(orbit.shape, jnp.float32)
        for block in range(N_CHOL):
            lower = block * PTS_DEV
            piece = jnp.dot(mixed[:, lower:lower + PTS_DEV], interp[:, lower:lower + PTS_DEV].T, preferred_element_type=jnp.float32)
            rounded = lax.optimization_barrier(piece.astype(jnp.bfloat16))
            summed = summed + rounded.astype(jnp.float32)
        term = summed.astype(jnp.bfloat16)
        total = total + term.astype(jnp.float32)
    return total.astype(jnp.bfloat16), bias


def reference(orbitals, intersection_inv, interp, occ_interp, chol_factors, fields):
    def single(items):
        return propagate(items[0], items[1], items[2], interp, occ_interp, chol_factors)

    new_orbitals, force_bias = lax.map(single, (orbitals, intersection_inv, fields))
    return (new_orbitals, force_bias)
```

```python
import functools

import jax
import jax.numpy as jnp
from jax import lax
from jax.experimental import pallas as pl
from jax.experimental.pallas import tpu as pltpu
from jax.sharding import PartitionSpec as P

TERMS = 4
TILE = 16
CHUNKS = 4
EARLY = 1
MESH = pl.DeviceIdType.MESH

time_root = 2.2


def split_dot(a, b, dims):
    high = a.astype(jnp.bfloat16)
    rest = a - high.astype(jnp.float32)
    middle = rest.astype(jnp.bfloat16)
    low = (rest - middle.astype(jnp.float32)).astype(jnp.bfloat16)
    dot = functools.partial(
        lax.dot_general, dimension_numbers=(dims, ((), ())), preferred_element_type=jnp.float32
    )
    return dot(high, b) + (dot(middle, b) + dot(low, b))


def kernel(
    nw, nc, stride,
    orb, inv, interp, occ, fac, fld,
    out, bias_out,
    full, orbs, invv, occv, facv, fldv, term, acc, total, outb,
    wrow, allw, wmat, bpart, frow, crow, scal,
    loc, osib, oy, ofw, ysem, p1, p2, p3, sibo, sibs, asem, bsem, csem, dsem, esem,
):
    me_w = lax.axis_index("walk")
    me_c = lax.axis_index("chol")
    ny = nc // 2
    core = lax.rem(me_c, 2)
    y = me_c // 2
    sib = me_c + 1 - 2 * core
    basis, pts = interp.shape
    rows = orb.shape[0]
    own = (rows // TILE) // nc * TILE
    tail = rows - own * nc
    piece = basis // 4
    size = piece // CHUNKS

    bit_x = lax.rem(me_w, 2)
    bit_z = lax.rem(me_w // stride, 2)
    w_x = me_w + 1 - 2 * bit_x
    w_z = me_w + stride * (1 - 2 * bit_z)
    w_1 = w_x + core * (w_z - w_x)
    w_2 = w_z + core * (w_x - w_z)
    j_0 = 2 * bit_z + bit_x
    j_x = 2 * bit_z + 1 - bit_x
    j_z = 2 * (1 - bit_z) + bit_x
    j_1 = j_x + core * (j_z - j_x)
    j_2 = j_z + core * (j_x - j_z)
    pieces = (j_0, j_1, j_2, 3 - j_0)

    def send(src, dst, sems, index, w, c):
        return pltpu.make_async_remote_copy(
            src_ref=src, dst_ref=dst, send_sem=sems.at[(0,) + index], recv_sem=sems.at[(1,) + index],
            device_id=(w, c), device_id_type=MESH,
        )

    def chunk(stage, q):
        return pl.ds(pl.multiple_of(pieces[stage] * piece + q * size, size), size)

    def walk_peer(d):
        return lax.rem(me_w + d, nw)

    def chol_peer(d):
        return lax.rem(me_c + d, nc)

    local = [
        pltpu.make_async_copy(src, dst, loc.at[n])
        for n, (src, dst) in enumerate((
            (interp, full.at[me_c]), (orb, orbs.at[me_c]), (inv, invv), (occ, occv), (fac, facv), (fld, fldv),
        ))
    ]
    for copy in local:
        copy.start()

    barrier = pltpu.get_barrier_semaphore()
    for d in range(1, nw):
        pl.semaphore_signal(barrier, inc=1, device_id=(walk_peer(d), me_c), device_id_type=MESH)
    for d in range(1, nc):
        pl.semaphore_signal(barrier, inc=1, device_id=(me_w, chol_peer(d)), device_id_type=MESH)
    pl.semaphore_wait(barrier, nw + nc - 2)

    pending = []

    def go(copy):
        copy.start()
        pending.append(copy)
        return copy

    y_copies = {}

    def start_y(q):
        for d in range(1, ny):
            target = lax.rem(y + d, ny) * 2 + core
            at = chunk(0, q)
            y_copies[d, q] = go(send(interp.at[at], full.at[me_c, at], ysem, (d - 1, q), me_w, target))

    for q in range(EARLY):
        start_y(q)
    half = (rows // TILE + 1) // 2 * TILE
    parts = (pl.ds(0, half), pl.ds(half, rows - half))
    orb_y = {}
    for h, part in enumerate(parts):
        for d in range(1, ny):
            target = lax.rem(y + d, ny) * 2 + core
            orb_y[d, h] = go(send(orb.at[part], orbs.at[me_c, part], oy, (d - 1, h), me_w, target))
    orb_sib = go(send(orb, orbs.at[me_c], osib, (0,), me_w, sib))
    for q in range(EARLY, CHUNKS):
        start_y(q)
    own_sib = go(send(interp, full.at[me_c], sibo, (0,), me_w, sib))

    sib_copies = []

    def to_sibling(d, stage, q, block, at):
        copy = go(send(full.at[block, at], full.at[block, at], sibs, (d - 1, stage, q), me_w, sib))
        sib_copies.append(copy)

    first, second, third = {}, {}, {}

    def forward(stage, q):
        for d in range(1, ny):
            block = lax.rem(y - d + ny, ny) * 2 + core
            at = chunk(stage, q)
            place = full.at[block, at]
            if stage == 0:
                y_copies[d, q].wait_recv()
                first[d, q] = go(send(place, place, p1, (d - 1, q), w_1, me_c))
                second[d, q] = go(send(place, place, p2, (d - 1, q), w_2, me_c))
            elif stage == 1:
                first[d, q].wait_recv()
                third[d, q] = go(send(place, place, p3, (d - 1, q), w_2, me_c))
            elif stage == 2:
                second[d, q].wait_recv()
            else:
                third[d, q].wait_recv()
            to_sibling(d, stage, q, block, at)

    for q in range(EARLY):
        forward(0, q)

    orb_fw = []
    for h, part in enumerate(parts):
        for d in range(1, ny):
            block = lax.rem(y - d + ny, ny) * 2 + core
            orb_y[d, h].wait_recv()
            place = orbs.at[block, part]
            orb_fw.append(go(send(place, place, ofw, (d - 1, h), me_w, sib)))
    for copy in local:
        copy.wait()
    orb_sib.wait_recv()
    for copy in orb_fw:
        copy.wait_recv()

    applied = jnp.zeros((rows, pts), jnp.float32)
    depth = orb.shape[1]
    for c in range(nc):
        applied += jnp.dot(
            orbs[c], full[me_c, c * depth:(c + 1) * depth, :], preferred_element_type=jnp.float32
        )
    projected = jnp.dot(invv[...], applied.astype(jnp.bfloat16), preferred_element_type=jnp.float32)
    wrow[0] = jnp.sum(occv[...].astype(jnp.float32) * projected, axis=0, keepdims=True)
    allw[pl.ds(me_w, 1)] = wrow[...]
    a_copies = [
        go(send(wrow.at[0], allw.at[me_w], asem, (d - 1,), walk_peer(d), me_c)) for d in range(1, nw)
    ]

    for q in range(EARLY):
        forward(1, q)
        forward(2, q)
    forward(0, EARLY)

    for copy in a_copies:
        copy.wait_recv()
    for w in range(nw):
        wmat[w:w + 1, :] = allw[w]
    bpart[pl.ds(me_c, 1)] = split_dot(wmat[...], facv[...], ((1,), (0,)))[None]
    b_copies = [
        go(send(bpart.at[me_c], bpart.at[me_c], bsem, (d - 1,), me_w, chol_peer(d))) for d in range(1, nc)
    ]

    forward(0, EARLY + 1)
    for copy in b_copies:
        copy.wait_recv()
    bias = bpart[0]
    for c in range(1, nc):
        bias = bias + bpart[c]
    bias_out[...] = bias
    coeff = time_root * (fldv[...] - bias)
    part_scales = split_dot(coeff, facv[...], ((1,), (1,)))
    for w in range(nw):
        frow[w] = part_scales[w:w + 1, :]
    crow[pl.ds(me_w, 1)] = frow[pl.ds(me_w, 1)]
    c_copies = [
        go(send(frow.at[walk_peer(d)], crow.at[me_w], csem, (d - 1,), walk_peer(d), me_c))
        for d in range(1, nw)
    ]

    for q in range(EARLY, CHUNKS):
        if q > EARLY + 1:
            forward(0, q)
        forward(1, q)
        forward(2, q)
    for q in range(CHUNKS):
        forward(3, q)

    for copy in c_copies:
        copy.wait_recv()
    row = crow[0]
    for w in range(1, nw):
        row = row + crow[w]
    scal[pl.ds(me_c, 1)] = row[None]
    d_copies = [
        go(send(scal.at[me_c], scal.at[me_c], dsem, (d - 1,), me_w, chol_peer(d))) for d in range(1, nc)
    ]

    start = pl.multiple_of(me_c * own, TILE)
    for c in range(nc):
        columns = slice(c * depth, (c + 1) * depth)
        term[0:own, columns] = orbs[c, pl.ds(start, own), :]
        if tail:
            term[own:own + tail, columns] = orbs[c, own * nc:rows, :]
    total[...] = term[...].astype(jnp.float32)

    own_sib.wait_recv()
    for copy in d_copies:
        copy.wait_recv()
    for copy in sib_copies:
        copy.wait_recv()

    def taylor(order, carry):
        acc[...] = jnp.zeros_like(acc)
        inverse = 1.0 / (order + 1).astype(jnp.float32)

        def block(pb, carry):
            value = jnp.dot(term[...], full[pb], preferred_element_type=jnp.float32)
            mixed = (value * (scal[pb] * inverse)).astype(jnp.bfloat16)
            acc[...] += lax.dot_general(
                mixed, full[pb], (((1,), (1,)), ((), ())), preferred_element_type=jnp.float32
            )
            return carry

        lax.fori_loop(0, nc, block, 0)
        rounded = acc[...].astype(jnp.bfloat16)
        term[...] = rounded
        total[...] += rounded.astype(jnp.float32)
        return carry

    lax.fori_loop(0, TERMS, taylor, 0)

    for c in range(nc):
        outb[c] = total[:, c * depth:(c + 1) * depth].astype(jnp.bfloat16)
    mine = pl.ds(start, own)
    e_copies = [
        go(send(outb.at[chol_peer(d), 0:own], out.at[mine], esem, (d - 1,), me_w, chol_peer(d)))
        for d in range(1, nc)
    ]
    out[mine, :] = outb[me_c, 0:own, :]
    if tail:
        out[own * nc:rows, :] = outb[me_c, own:own + tail, :]
    for copy in e_copies:
        copy.wait_recv()
    for copy in pending:
        copy.wait_send()


def solution(mesh):
    nw, nc = mesh.shape["walk"], mesh.shape["chol"]
    stride = 2 ** ((nw.bit_length() - 1) // 2)

    def on_device(orbitals, intersection_inv, interp, occ_interp, chol_factors, fields):
        _, rows, depth = orbitals.shape
        basis, pts = interp.shape
        vecs = chol_factors.shape[1]
        ny = nc // 2
        links = max(ny - 1, 1)
        own = (rows // TILE) // nc * TILE
        held = own + rows - own * nc
        f32, bf16 = jnp.float32, jnp.bfloat16
        dma = pltpu.SemaphoreType.DMA
        anywhere = pl.BlockSpec(memory_space=pl.ANY)
        vmem = pl.BlockSpec(memory_space=pltpu.VMEM)
        new, bias = pl.pallas_call(
            functools.partial(kernel, nw, nc, stride),
            out_shape=(
                jax.ShapeDtypeStruct((rows, depth), bf16),
                jax.ShapeDtypeStruct((nw, vecs), f32),
            ),
            in_specs=[anywhere] * 6,
            out_specs=(vmem, vmem),
            scratch_shapes=[
                pltpu.VMEM((nc, basis, pts), bf16),
                pltpu.VMEM((nc, rows, depth), bf16),
                pltpu.VMEM((rows, rows), bf16),
                pltpu.VMEM((rows, pts), bf16),
                pltpu.VMEM((pts, vecs), bf16),
                pltpu.VMEM((nw, vecs), f32),
                pltpu.VMEM((held, basis), bf16),
                pltpu.VMEM((held, basis), f32),
                pltpu.VMEM((held, basis), f32),
                pltpu.VMEM((nc, held, depth), bf16),
                pltpu.VMEM((1, 1, pts), f32),
                pltpu.VMEM((nw, 1, pts), f32),
                pltpu.VMEM((nw, pts), f32),
                pltpu.VMEM((nc, nw, vecs), f32),
                pltpu.VMEM((nw, 1, pts), f32),
                pltpu.VMEM((nw, 1, pts), f32),
                pltpu.VMEM((nc, 1, pts), f32),
                dma((6,)),
                dma((2, 1)),
                dma((2, links, 2)),
                dma((2, links, 2)),
                dma((2, links, CHUNKS)),
                dma((2, links, CHUNKS)),
                dma((2, links, CHUNKS)),
                dma((2, links, CHUNKS)),
                dma((2, 1)),
                dma((2, links, 4, CHUNKS)),
                dma((2, nw - 1)),
                dma((2, nc - 1)),
                dma((2, nw - 1)),
                dma((2, nc - 1)),
                dma((2, nc - 1)),
            ],
            compiler_params=pltpu.CompilerParams(
                collective_id=0, has_side_effects=True, vmem_limit_bytes=60 * 2**20
            ),
        )(orbitals[0], intersection_inv[0], interp, occ_interp, chol_factors, fields)
        return new[None], bias

    placed = (
        P("walk", None, "chol"),
        P("walk", None, None),
        P(None, "chol"),
        P(None, "chol"),
        P("chol", "walk"),
        P(None, "walk"),
    )
    return jax.shard_map(
        on_device,
        mesh=mesh,
        in_specs=placed,
        out_specs=(P("walk", None, "chol"), P(None, "walk")),
        check_vma=False,
    )
```

```python
import functools

import jax
import jax.numpy as jnp
from jax import lax
from jax.experimental import pallas as pl
from jax.experimental.pallas import tpu as pltpu
from jax.sharding import PartitionSpec as P

TERMS = 4
TILE = 16
CHUNKS = 4
EARLY = 3
LAG = 1
CUTS = (9, 12, 13, 16)
MESH = pl.DeviceIdType.MESH

time_root = 2.2


def split_dot(a, b, dims):
    high = a.astype(jnp.bfloat16)
    rest = a - high.astype(jnp.float32)
    middle = rest.astype(jnp.bfloat16)
    low = (rest - middle.astype(jnp.float32)).astype(jnp.bfloat16)
    dot = functools.partial(
        lax.dot_general, dimension_numbers=(dims, ((), ())), preferred_element_type=jnp.float32
    )
    return dot(high, b) + (dot(middle, b) + dot(low, b))


def kernel(
    nw, nc, stride,
    orb, inv, interp, occ, fac, fld,
    out, bias_out,
    full, flip, orbs, invv, occv, facv, fldv, term, value, mixed, total, outb,
    wrow, allw, wmat, bpart, frow, crow, scal,
    loc, osib, oy, ofw, ysem, p1, p2, p3, sibo, sibs, asem, bsem, csem, dsem, esem,
):
    me_w = lax.axis_index("walk")
    me_c = lax.axis_index("chol")
    ny = nc // 2
    core = lax.rem(me_c, 2)
    y = me_c // 2
    sib = me_c + 1 - 2 * core
    basis, pts = interp.shape
    rows = orb.shape[0]
    own = (rows // TILE) // nc * TILE
    tail = rows - own * nc
    piece = basis // 4
    size = piece // CHUNKS

    bit_x = lax.rem(me_w, 2)
    bit_z = lax.rem(me_w // stride, 2)
    w_x = me_w + 1 - 2 * bit_x
    w_z = me_w + stride * (1 - 2 * bit_z)
    w_1 = w_x + core * (w_z - w_x)
    w_2 = w_z + core * (w_x - w_z)
    j_0 = 2 * bit_z + bit_x
    j_x = 2 * bit_z + 1 - bit_x
    j_z = 2 * (1 - bit_z) + bit_x
    j_1 = j_x + core * (j_z - j_x)
    j_2 = j_z + core * (j_x - j_z)
    pieces = (j_0, j_1, j_2, 3 - j_0)

    def send(src, dst, sems, index, w, c):
        return pltpu.make_async_remote_copy(
            src_ref=src, dst_ref=dst, send_sem=sems.at[(0,) + index], recv_sem=sems.at[(1,) + index],
            device_id=(w, c), device_id_type=MESH,
        )

    def chunk(stage, q):
        return pl.ds(pl.multiple_of(pieces[stage] * piece + q * size, size), size)

    def walk_peer(d):
        return lax.rem(me_w + d, nw)

    def chol_peer(d):
        return lax.rem(me_c + d, nc)

    local = [
        pltpu.make_async_copy(src, dst, loc.at[n])
        for n, (src, dst) in enumerate((
            (interp, full.at[me_c]), (orb, orbs.at[me_c]), (inv, invv), (occ, occv), (fac, facv), (fld, fldv),
        ))
    ]
    for copy in local:
        copy.start()

    barrier = pltpu.get_barrier_semaphore()
    for d in range(1, nw):
        pl.semaphore_signal(barrier, inc=1, device_id=(walk_peer(d), me_c), device_id_type=MESH)
    for d in range(1, nc):
        pl.semaphore_signal(barrier, inc=1, device_id=(me_w, chol_peer(d)), device_id_type=MESH)
    pl.semaphore_wait(barrier, nw + nc - 2)

    pending = []

    def go(copy):
        copy.start()
        pending.append(copy)
        return copy

    y_copies = {}

    def start_y(q):
        for d in range(1, ny):
            target = lax.rem(y + d, ny) * 2 + core
            at = chunk(0, q)
            y_copies[d, q] = go(send(interp.at[at], full.at[me_c, at], ysem, (d - 1, q), me_w, target))

    for q in range(EARLY):
        start_y(q)
    half = (rows // TILE + 1) // 2 * TILE
    parts = (pl.ds(0, half), pl.ds(half, rows - half))
    orb_y = {}
    for h, part in enumerate(parts):
        for d in range(1, ny):
            target = lax.rem(y + d, ny) * 2 + core
            orb_y[d, h] = go(send(orb.at[part], orbs.at[me_c, part], oy, (d - 1, h), me_w, target))
    orb_sib = go(send(orb, orbs.at[me_c], osib, (0,), me_w, sib))
    for q in range(EARLY, CHUNKS):
        start_y(q)
    own_sib = go(send(interp, full.at[me_c], sibo, (0,), me_w, sib))

    sib_copies = []

    def to_sibling(d, stage, q, block, at):
        copy = go(send(full.at[block, at], full.at[block, at], sibs, (d - 1, stage, q), me_w, sib))
        sib_copies.append(copy)

    first, second, third = {}, {}, {}

    def forward(stage, q):
        for d in range(1, ny):
            block = lax.rem(y - d + ny, ny) * 2 + core
            at = chunk(stage, q)
            place = full.at[block, at]
            if stage == 0:
                y_copies[d, q].wait_recv()
                first[d, q] = go(send(place, place, p1, (d - 1, q), w_1, me_c))
                second[d, q] = go(send(place, place, p2, (d - 1, q), w_2, me_c))
            elif stage == 1:
                first[d, q].wait_recv()
                third[d, q] = go(send(place, place, p3, (d - 1, q), w_2, me_c))
            elif stage == 2:
                second[d, q].wait_recv()
            else:
                third[d, q].wait_recv()
            to_sibling(d, stage, q, block, at)

    steps = []
    for t in range(CHUNKS + 2):
        for stage, q in ((0, t), (1, t - 1), (2, t - 1), (3, t - 1 - LAG)):
            if 0 <= q < CHUNKS:
                steps.append((stage, q))
    steps += [(3, q) for q in range(CHUNKS) if (3, q) not in steps]
    steps.sort(key=lambda step: not (step[1] < EARLY and step[0] < 3))

    def forward_until(count):
        while steps and len(steps) > 4 * CHUNKS - count:
            forward(*steps.pop(0))

    forward_until(CUTS[0])

    orb_fw = []
    for h, part in enumerate(parts):
        for d in range(1, ny):
            block = lax.rem(y - d + ny, ny) * 2 + core
            orb_y[d, h].wait_recv()
            place = orbs.at[block, part]
            orb_fw.append(go(send(place, place, ofw, (d - 1, h), me_w, sib)))
    for copy in local:
        copy.wait()
    orb_sib.wait_recv()
    for copy in orb_fw:
        copy.wait_recv()

    applied = jnp.zeros((rows, pts), jnp.float32)
    depth = orb.shape[1]
    for c in range(nc):
        applied += jnp.dot(
            orbs[c], full[me_c, c * depth:(c + 1) * depth, :], preferred_element_type=jnp.float32
        )
    projected = jnp.dot(invv[...], applied.astype(jnp.bfloat16), preferred_element_type=jnp.float32)
    wrow[0] = jnp.sum(occv[...].astype(jnp.float32) * projected, axis=0, keepdims=True)
    allw[pl.ds(me_w, 1)] = wrow[...]
    a_copies = [
        go(send(wrow.at[0], allw.at[me_w], asem, (d - 1,), walk_peer(d), me_c)) for d in range(1, nw)
    ]

    forward_until(CUTS[1])
    for c in range(nc):
        span = slice(c * depth, (c + 1) * depth)
        flip[0, :, span] = full[me_c, span, :].T

    for copy in a_copies:
        copy.wait_recv()
    for w in range(nw):
        wmat[w:w + 1, :] = allw[w]
    bpart[pl.ds(me_c, 1)] = split_dot(wmat[...], facv[...], ((1,), (0,)))[None]
    b_copies = [
        go(send(bpart.at[me_c], bpart.at[me_c], bsem, (d - 1,), me_w, chol_peer(d))) for d in range(1, nc)
    ]

    forward_until(CUTS[2])
    own_sib.wait_recv()
    for c in range(nc):
        span = slice(c * depth, (c + 1) * depth)
        flip[1, :, span] = full[sib, span, :].T
    for copy in b_copies:
        copy.wait_recv()
    bias = bpart[0]
    for c in range(1, nc):
        bias = bias + bpart[c]
    bias_out[...] = bias
    coeff = time_root * (fldv[...] - bias)
    part_scales = split_dot(coeff, facv[...], ((1,), (1,)))
    for w in range(nw):
        frow[w] = part_scales[w:w + 1, :]
    crow[pl.ds(me_w, 1)] = frow[pl.ds(me_w, 1)]
    c_copies = [
        go(send(frow.at[walk_peer(d)], crow.at[me_w], csem, (d - 1,), walk_peer(d), me_c))
        for d in range(1, nw)
    ]

    forward_until(CUTS[3])

    start = pl.multiple_of(me_c * own, TILE)
    for c in range(nc):
        columns = slice(c * depth, (c + 1) * depth)
        term[0:own, columns] = orbs[c, pl.ds(start, own), :]
        if tail:
            term[own:own + tail, columns] = orbs[c, own * nc:rows, :]
    total[...] = term[...].astype(jnp.float32)

    forward_until(4 * CHUNKS)
    for copy in sib_copies:
        copy.wait_recv()

    def open_block(pb, carry):
        value[pb] = jnp.dot(term[...], full[pb], preferred_element_type=jnp.float32)
        return carry

    lax.fori_loop(0, nc, open_block, 0)

    for copy in c_copies:
        copy.wait_recv()
    row = crow[0]
    for w in range(1, nw):
        row = row + crow[w]
    scal[pl.ds(me_c, 1)] = row[None]
    d_copies = [
        go(send(scal.at[me_c], scal.at[me_c], dsem, (d - 1,), me_w, chol_peer(d))) for d in range(1, nc)
    ]
    for copy in d_copies:
        copy.wait_recv()

    def mix(pb, order):
        mixed[pb] = (value[pb] * (scal[pb] * (1.0 / order))).astype(jnp.bfloat16)

    def back(mb):
        at = pl.ds(pl.multiple_of(mb * depth, depth), depth)
        result = jnp.zeros((term.shape[0], depth), jnp.float32)
        for n, pb in enumerate((me_c, sib)):
            result += jnp.dot(mixed[pb], flip[n, :, at], preferred_element_type=jnp.float32)
        for d, e in [(d, e) for d in range(1, ny) for e in (0, 1)]:
            pb = lax.rem(y + d, ny) * 2 + e
            result += lax.dot_general(
                mixed[pb], full[pb, at, :], (((1,), (1,)), ((), ())), preferred_element_type=jnp.float32
            )
        rounded = result.astype(jnp.bfloat16)
        term[:, at] = rounded
        summed = total[:, at] + rounded.astype(jnp.float32)
        total[:, at] = summed
        return summed

    for pb in range(nc):
        mix(pb, jnp.float32(1.0))

    def taylor(order, carry):
        def back_block(mb, carry):
            back(mb)
            return carry

        def block(pb, carry):
            value[pb] = jnp.dot(term[...], full[pb], preferred_element_type=jnp.float32)
            mix(pb, order.astype(jnp.float32))
            return carry

        lax.fori_loop(0, nc, back_block, 0)
        lax.fori_loop(0, nc, block, 0)
        return carry

    lax.fori_loop(2, TERMS + 1, taylor, 0)

    mine = pl.ds(start, own)
    e_copies = []
    hops = [(d, e) for d in range(1, ny) for e in (0, 1)] + [(0, 1), (0, 0)]
    for n, (d, e) in enumerate(hops):
        c = lax.rem(y + d, ny) * 2 + (core if e == 0 else 1 - core)
        outb[n] = back(c).astype(jnp.bfloat16)
        if n < nc - 1:
            e_copies.append(go(send(outb.at[n, 0:own], out.at[mine], esem, (n,), me_w, c)))
    out[mine, :] = outb[nc - 1, 0:own, :]
    if tail:
        out[own * nc:rows, :] = outb[nc - 1, own:own + tail, :]
    for copy in e_copies:
        copy.wait_recv()
    for copy in pending:
        copy.wait_send()


def solution(mesh):
    nw, nc = mesh.shape["walk"], mesh.shape["chol"]
    stride = 2 ** ((nw.bit_length() - 1) // 2)

    def on_device(orbitals, intersection_inv, interp, occ_interp, chol_factors, fields):
        _, rows, depth = orbitals.shape
        basis, pts = interp.shape
        vecs = chol_factors.shape[1]
        ny = nc // 2
        links = max(ny - 1, 1)
        own = (rows // TILE) // nc * TILE
        held = own + rows - own * nc
        f32, bf16 = jnp.float32, jnp.bfloat16
        dma = pltpu.SemaphoreType.DMA
        anywhere = pl.BlockSpec(memory_space=pl.ANY)
        vmem = pl.BlockSpec(memory_space=pltpu.VMEM)
        new, bias = pl.pallas_call(
            functools.partial(kernel, nw, nc, stride),
            out_shape=(
                jax.ShapeDtypeStruct((rows, depth), bf16),
                jax.ShapeDtypeStruct((nw, vecs), f32),
            ),
            in_specs=[anywhere] * 6,
            out_specs=(vmem, vmem),
            scratch_shapes=[
                pltpu.VMEM((nc, basis, pts), bf16),
                pltpu.VMEM((2, pts, basis), bf16),
                pltpu.VMEM((nc, rows, depth), bf16),
                pltpu.VMEM((rows, rows), bf16),
                pltpu.VMEM((rows, pts), bf16),
                pltpu.VMEM((pts, vecs), bf16),
                pltpu.VMEM((nw, vecs), f32),
                pltpu.VMEM((held, basis), bf16),
                pltpu.VMEM((nc, held, pts), f32),
                pltpu.VMEM((nc, held, pts), bf16),
                pltpu.VMEM((held, basis), f32),
                pltpu.VMEM((nc, held, depth), bf16),
                pltpu.VMEM((1, 1, pts), f32),
                pltpu.VMEM((nw, 1, pts), f32),
                pltpu.VMEM((nw, pts), f32),
                pltpu.VMEM((nc, nw, vecs), f32),
                pltpu.VMEM((nw, 1, pts), f32),
                pltpu.VMEM((nw, 1, pts), f32),
                pltpu.VMEM((nc, 1, pts), f32),
                dma((6,)),
                dma((2, 1)),
                dma((2, links, 2)),
                dma((2, links, 2)),
                dma((2, links, CHUNKS)),
                dma((2, links, CHUNKS)),
                dma((2, links, CHUNKS)),
                dma((2, links, CHUNKS)),
                dma((2, 1)),
                dma((2, links, 4, CHUNKS)),
                dma((2, nw - 1)),
                dma((2, nc - 1)),
                dma((2, nw - 1)),
                dma((2, nc - 1)),
                dma((2, nc - 1)),
            ],
            compiler_params=pltpu.CompilerParams(
                collective_id=0, has_side_effects=True, vmem_limit_bytes=60 * 2**20
            ),
        )(orbitals[0], intersection_inv[0], interp, occ_interp, chol_factors, fields)
        return new[None], bias

    placed = (
        P("walk", None, "chol"),
        P("walk", None, None),
        P(None, "chol"),
        P(None, "chol"),
        P("chol", "walk"),
        P(None, "walk"),
    )
    return jax.shard_map(
        on_device,
        mesh=mesh,
        in_specs=placed,
        out_specs=(P("walk", None, "chol"), P(None, "walk")),
        check_vma=False,
    )
```
